32 devices in a mesh: ep: 8 (over y, x, core), tp: 4 (over z).
Axes of the slice: x: 2, y: 2, z: 4, core: 2. Of those that a mesh axis runs over, the one named last changes fastest.
Arguments:
- tokens: bfloat16 [4096, 2048], P('ep'), may hold values from -6 to 6
- lengths: int32 [8], P('ep'), may hold values from 256 to 512, as said below
- routes: int32 [4096, 4], P('ep'), may hold values from 0 to 7, all different within a row; in each aligned block of 512 rows (0 to 511, 512 to 1023, ...) at most 384 rows name the same one
- attention_gain: bfloat16 [2048], P('ep'), may hold values from 0.5 to 1.5
- query_weight: bfloat16 [2048, 2048], P('ep', 'tp'), may hold values from -0.125 to 0.125
- key_weight: bfloat16 [2048, 2048], P('ep', 'tp'), may hold values from -0.125 to 0.125
- value_weight: bfloat16 [2048, 2048], P('ep', 'tp'), may hold values from -0.125 to 0.125
- query_bias: bfloat16 [16, 128], P('tp', 'ep'), may hold values from -0.59765625 to 0.59765625
- key_bias: bfloat16 [16, 128], P('tp', 'ep'), may hold values from -0.59765625 to 0.59765625
- value_bias: bfloat16 [16, 128], P('tp', 'ep'), may hold values from -0.59765625 to 0.59765625
- output_weight: bfloat16 [2048, 2048], P('tp', 'ep'), may hold values from -0.5 to 0.5
- feedforward_gain: bfloat16 [2048], P('ep'), may hold values from 0.5 to 1.5
- router_weight: bfloat16 [2048, 8], P('ep'), may hold values from -0.0625 to 0.0625
- shared_switch: bfloat16 [2048], P('ep'), may hold values from -0.125 to 0.125
- shared_gate: bfloat16 [2048, 5632], P('ep', 'tp'), may hold values from -0.125 to 0.125
- shared_up: bfloat16 [2048, 5632], P('ep', 'tp'), may hold values from -0.125 to 0.125
- shared_down: bfloat16 [5632, 2048], P('tp', 'ep'), may hold values from -0.21875 to 0.21875
- expert_gate: bfloat16 [8, 2048, 1408], P('ep', None, 'tp'), may hold values from -0.125 to 0.125
- expert_up: bfloat16 [8, 2048, 1408], P('ep', None, 'tp'), may hold values from -0.125 to 0.125
- expert_down: bfloat16 [8, 1408, 2048], P('ep', 'tp'), may hold values from -1.25 to 1.25
- cotangent: bfloat16 [4096, 2048], P('ep'), may hold values from -6 to 6
Outputs:
- output: bfloat16 [4096, 2048], P('ep')
- aux_loss: float32 [], replicated
- expert_load: float32 [8], replicated
- tokens_grad: float32 [4096, 2048], P('ep')
- attention_gain_grad: float32 [2048], P('ep')
- query_weight_grad: float32 [2048, 2048], P('ep', 'tp')
- key_weight_grad: float32 [2048, 2048], P('ep', 'tp')
- value_weight_grad: float32 [2048, 2048], P('ep', 'tp')
- query_bias_grad: float32 [16, 128], P('tp', 'ep')
- key_bias_grad: float32 [16, 128], P('tp', 'ep')
- value_bias_grad: float32 [16, 128], P('tp', 'ep')
- output_weight_grad: float32 [2048, 2048], P('tp', 'ep')
- feedforward_gain_grad: float32 [2048], P('ep')
- router_weight_grad: float32 [2048, 8], P('ep')
- shared_switch_grad: float32 [2048], P('ep')
- shared_gate_grad: float32 [2048, 5632], P('ep', 'tp')
- shared_up_grad: float32 [2048, 5632], P('ep', 'tp')
- shared_down_grad: float32 [5632, 2048], P('tp', 'ep')
- expert_gate_grad: float32 [8, 2048, 1408], P('ep', None, 'tp')
- expert_up_gradient: float32 [8, 2048, 1408], P('ep', None, 'tp')
- expert_down_grad: float32 [8, 1408, 2048], P('ep', 'tp')
The draws below stay inside these ranges and needn't reach their ends.
Inputs may be any that keep to these rules, and one draw needn't show every extreme that they name: `lengths`: every sequence has at least 256 tokens in use; in every draw one sequence is full and one has exactly 256. `routes`: A token names 4 different experts; among the 512 tokens of one sequence no expert is named more than 384 times, and in every draw some expert is named exactly 384 times by some sequence.
All inputs are finite; a program needn't handle non-finite values.
Results may differ from the reference program's by a relative error of at most 0.028.
Values may be sent and summed in bfloat16 or wider, within the bound.
A program may use at most 256 MiB of HBM per device.

```python
import math
import jax
import jax.numpy as jnp
import numpy as np
from jax import lax

D = 2048
H = 16
HD = 128
EFF = 1408
SFF = 5632
TOP = 4
SLOT = 512
EXPERTS = 8
CAP = 384
SEQS = 8
TOKENS = 4096
N_EP = 8


def draw_lengths(key, part):
    base = jax.random.randint(jax.random.fold_in(key, 11), (SEQS,), SLOT // 2, SLOT + 1)
    first = jax.random.randint(jax.random.fold_in(key, 12), (), 0, SEQS)
    offset = jax.random.randint(jax.random.fold_in(key, 13), (), 1, SEQS)
    second = (first + offset) % SEQS
    positions = jnp.arange(SEQS)
    base = jnp.where(positions == first, SLOT, base)
    base = jnp.where(positions == second, SLOT // 2, base)
    return base.astype(jnp.int32)


def shard_levels(key, shape, cuts, least, high):
    factor_of, own = 1.0, jax.random.fold_in(key, 6)
    for dim, shards_of in cuts:
        draws = jnp.exp(jax.random.uniform(jax.random.fold_in(own, dim), (shards_of,), jnp.float32, least / len(cuts), high / len(cuts)))
        factor_of = factor_of * jnp.repeat(draws, shape[dim] // shards_of).reshape([-1 if axis == dim else 1 for axis in range(len(shape))])
    return factor_of


def assign_block(rng, own, number, rows, count, top, most, skew):
    ranking = jax.random.permutation(rng, count)
    crowded, ordinary = load_shares(count, rows * top, most, skew, True), load_shares(count, rows * top, most, skew, False)
    places = jnp.arange(count)

    def named(sizes, rotation):
        used = int((sizes > 0).sum())
        fixed = max(1, used // 4)
        moved = fixed + (places - fixed + rotation * (used - fixed)) % max(1, count - fixed)
        return jnp.zeros((count,), jnp.int32).at[ranking[jnp.where(places < fixed, places, moved)]].set(jnp.asarray(sizes, jnp.int32))

    sizes = jnp.where(number % 4 == 0, named(crowded, number // 4), named(ordinary, number - number // 4 - 1))
    mixed = jax.random.permutation(jax.random.fold_in(own, 3), count)
    donor, receiver = mixed[0:count // 2 * 2:2], mixed[1:count // 2 * 2:2]
    slack = jnp.minimum(sizes[donor] - 1, most - sizes[receiver]) // 2
    slack = jnp.where((donor == ranking[0]) | (receiver == ranking[0]) | (sizes[receiver] == 0), 0, jnp.maximum(slack, 0))
    moved = jax.random.randint(jax.random.fold_in(own, 4), (count // 2,), 0, 1 << 20) % (slack + 1)
    sizes = sizes.at[donor].add(-moved).at[receiver].add(moved)
    members = jnp.searchsorted(jnp.cumsum(sizes), jnp.arange(rows * top), side="right").astype(jnp.int32)
    grid = members.reshape(top, rows).T
    grid = grid[jax.random.permutation(jax.random.fold_in(own, 1), rows)]
    rotation = jax.random.randint(jax.random.fold_in(own, 2), (rows, 1), 0, top)
    return jnp.take_along_axis(grid, (jnp.arange(top)[None, :] + rotation) % top, axis=1)


def load_shares(amount, total, limit, slope, full):
    portions = [(1 << 20) // math.isqrt(rank ** slope) + 1 for rank in range(1, amount + 1)]
    largest = limit if full else min(limit, max(-(-total // amount), total * portions[0] // sum(portions)))
    least = 1 if total - largest >= amount - 1 else 0
    holding, spare = [largest] + [least] * (amount - 1), total - largest - least * (amount - 1)
    while spare > 0:
        free = [i for i in range(1, amount) if holding[i] < largest] or [i for i in range(1, amount) if holding[i] < limit]
        mass, remaining = sum([portions[i] for i in free]), spare
        for i in free:
            extra = min(limit - holding[i], max(1, remaining * portions[i] // mass), spare)
            holding[i] = holding[i] + extra
            spare = spare - extra
    return np.array(holding)


def scatter_about(rng, shape, deviation, limit, shards=(), kind=jnp.bfloat16):
    values = jax.random.normal(rng, shape, jnp.float32) * deviation
    if len(shards) > 0:
        values = shard_levels(rng, shape, shards, -0.22, 0.18) * values
    return jnp.clip(values, min=-limit, max=limit).astype(kind)


def setup_inputs(seed: int = 0) -> dict:
    streams_of = jax.random.split(jax.random.key(seed), 22)
    tokens = scatter_about(streams_of[0], (TOKENS, D), 1.0, 6.0, ((0, 8),))
    lengths = draw_lengths(jax.random.fold_in(streams_of[21], 71), 0)
    routes_keys = jax.random.split(jax.random.fold_in(streams_of[2], 1), TOKENS // SLOT)
    routes_turns = jax.random.permutation(jax.random.fold_in(streams_of[2], 3), TOKENS // SLOT)
    routes = jax.vmap(lambda own, number: assign_block(jax.random.fold_in(streams_of[2], 2), own, number, SLOT, EXPERTS, TOP, CAP, 2))(routes_keys, routes_turns).reshape((TOKENS, TOP))
    attention_gain = jnp.clip(1.0 + 0.1 * jax.random.normal(streams_of[3], (D,), jnp.float32), 0.5, 1.5).astype(jnp.bfloat16)
    query_weight = scatter_about(streams_of[4], (D, H * HD), D ** -0.5, 0.125, ((0, 8), (1, 4)))
    key_weight = scatter_about(streams_of[5], (D, H * HD), D ** -0.5, 0.125, ((0, 8), (1, 4)))
    value_weight = scatter_about(streams_of[6], (D, H * HD), D ** -0.5, 0.125, ((0, 8), (1, 4)))
    query_bias = scatter_about(streams_of[7], (H, HD), 0.1, 0.59765625, ((0, 4), (1, 8)))
    key_bias = scatter_about(streams_of[8], (H, HD), 0.1, 0.59765625, ((0, 4), (1, 8)))
    value_bias = scatter_about(streams_of[9], (H, HD), 0.1, 0.59765625, ((0, 4), (1, 8)))
    output_weight = scatter_about(streams_of[10], (H * HD, D), (H * HD // 16) ** -0.5, 0.5, ((0, 4), (1, 8)))
    feedforward_gain = jnp.clip(1.0 + 0.1 * jax.random.normal(streams_of[11], (D,), jnp.float32), 0.5, 1.5).astype(jnp.bfloat16)
    router_weight = scatter_about(streams_of[12], (D, EXPERTS), (4 * D) ** -0.5, 0.0625, ((0, 8),))
    shared_switch = scatter_about(streams_of[13], (D,), D ** -0.5, 0.125, ((0, 8),))
    shared_gate = scatter_about(streams_of[14], (D, SFF), D ** -0.5, 0.125, ((0, 8), (1, 4)))
    shared_up = scatter_about(streams_of[15], (D, SFF), D ** -0.5, 0.125, ((0, 8), (1, 4)))
    shared_down = scatter_about(streams_of[16], (SFF, D), (SFF // 8) ** -0.5, 0.21875, ((0, 4), (1, 8)))
    expert_gate = scatter_about(streams_of[17], (EXPERTS, D, EFF), D ** -0.5, 0.125, ((0, 8), (2, 4)))
    expert_up = scatter_about(streams_of[18], (EXPERTS, D, EFF), D ** -0.5, 0.125, ((0, 8), (2, 4)))
    expert_down = scatter_about(streams_of[19], (EXPERTS, EFF, D), (max(EFF // (EXPERTS * EXPERTS), 1)) ** -0.5, 1.25, ((0, 8), (1, 4)))
    cotangent = scatter_about(streams_of[20], (TOKENS, D), 1.0, 6.0, ((0, 8),))
    return {"tokens": tokens, "lengths": lengths, "routes": routes, "attention_gain": attention_gain, "query_weight": query_weight, "key_weight": key_weight, "value_weight": value_weight, "query_bias": query_bias, "key_bias": key_bias, "value_bias": value_bias, "output_weight": output_weight, "feedforward_gain": feedforward_gain, "router_weight": router_weight, "shared_switch": shared_switch, "shared_gate": shared_gate, "shared_up": shared_up, "shared_down": shared_down, "expert_gate": expert_gate, "expert_up": expert_up, "expert_down": expert_down, "cotangent": cotangent}


@jax.custom_vjp
def low(v):
    return lax.optimization_barrier(v.astype(jnp.bfloat16)).astype(jnp.float32)

@jax.custom_vjp
def low_back(v):
    return v

def low_keep(v):
    return (low(v), None)

def low_pass(kept, grad):
    return (grad,)

def back_keep(v):
    return (v, None)

def back_low(kept, grad):
    return (low(grad),)
low.defvjp(low_keep, low_pass)
low_back.defvjp(back_keep, back_low)
epsilon = 1e-06
rope_base = 1000000.0
aux_weight = 0.001

def matmul(left, right):
    return jnp.dot(left, right, precision=lax.Precision.HIGHEST)

def rms_norm(values, gain):
    return values * lax.rsqrt(lax.optimization_barrier(jnp.mean(values * values, axis=-1, keepdims=True)) + epsilon) * gain

def rotary(values):
    half_size = HD // 2
    frequency = rope_base ** (-jnp.arange(half_size, dtype=jnp.float32) * 2.0 / HD)
    angles = jnp.arange(SLOT, dtype=jnp.float32)[:, None] * frequency[None, :]
    cosine = jnp.concatenate([jnp.cos(angles), jnp.cos(angles)], -1)[:, None, :]
    sine_table = jnp.concatenate([jnp.sin(angles), jnp.sin(angles)], -1)[:, None, :]
    turned = jnp.concatenate([-values[..., half_size:], values[..., :half_size]], -1)
    return values * cosine + turned * sine_table

def attend(queries, key_heads, value_heads, seq_length):
    scores = jnp.einsum('shd,thd->hst', queries, key_heads, precision=lax.Precision.HIGHEST) * HD ** (-0.5)
    scores = low_back(scores)
    positions = jnp.arange(SLOT, dtype=jnp.int32)
    keep_mask = (positions[None, :] <= positions[:, None]) & (positions[None, :] < seq_length)
    scores = jnp.where(keep_mask[None], scores, -1e+30)
    top_score = lax.optimization_barrier(jnp.max(scores, axis=-1, keepdims=True))
    exp_scores = jnp.exp(scores - top_score)
    weights = low(exp_scores / lax.optimization_barrier(jnp.sum(exp_scores, axis=-1, keepdims=True)))
    return jnp.einsum('hst,thd->shd', weights, value_heads, precision=lax.Precision.HIGHEST)

def expert_block(packed):
    rows_in, gate_matrix, up_weight_matrix, down_matrix = packed
    gate_pre = low_back(matmul(rows_in, gate_matrix))
    up_pre = low_back(matmul(rows_in, up_weight_matrix))
    inner_act = low(gate_pre * lax.logistic(gate_pre) * up_pre)
    return low_back(low(matmul(inner_act, down_matrix)))

def live_mask(lengths):
    positions = jnp.arange(SLOT, dtype=jnp.int32)
    return (positions[None, :] < lengths[:, None]).reshape(TOKENS).astype(jnp.float32)

def load_counts(routes, lengths):
    live_rows = live_mask(lengths)
    hot = (routes.astype(jnp.int32)[:, :, None] == jnp.arange(EXPERTS, dtype=jnp.int32)[None, None, :]).astype(jnp.float32)
    return lax.optimization_barrier(jnp.sum(live_rows[:, None] * lax.optimization_barrier(jnp.sum(hot, 1)), 0))

def forward(tokens_f, attention_gain, query_weight, key_weight, value_weight, query_bias, key_bias, value_bias, output_weight, feedforward_gain, router_weight, shared_switch, shared_gate, shared_up, shared_down, expert_gate, expert_up, expert_down, routes, lengths):
    live_rows = live_mask(lengths)
    attn_in = low(rms_norm(tokens_f, attention_gain))
    query_pre = low_back(matmul(attn_in, query_weight) + query_bias.reshape(-1))
    key_pre = low_back(matmul(attn_in, key_weight) + key_bias.reshape(-1))
    value_pre = low(low_back(matmul(attn_in, value_weight) + value_bias.reshape(-1)))
    head_shape = (SEQS, SLOT, H, HD)
    queries = low(rotary(query_pre.reshape(head_shape)))
    key_heads = low(rotary(key_pre.reshape(head_shape)))
    mixed_heads = jax.vmap(attend)(queries, key_heads, value_pre.reshape(head_shape), lengths)
    mixed_heads = low(low_back(mixed_heads.reshape(TOKENS, H * HD)))
    hidden_state = tokens_f + low_back(matmul(mixed_heads, output_weight))
    mlp_in = low(rms_norm(hidden_state, feedforward_gain))
    logits = low_back(matmul(mlp_in, router_weight))
    top_logit = lax.optimization_barrier(jnp.max(logits, axis=-1, keepdims=True))
    exp_logits = jnp.exp(logits - top_logit)
    router_probs = exp_logits / lax.optimization_barrier(jnp.sum(exp_logits, axis=-1, keepdims=True))
    flat_ids = routes.reshape(-1).astype(jnp.int32)
    flat_hot = (flat_ids[:, None] == jnp.arange(EXPERTS, dtype=jnp.int32)[None, :]).astype(jnp.int32)
    slot_rank = lax.optimization_barrier(jnp.sum((jnp.cumsum(flat_hot, 0).astype(jnp.int32) - flat_hot) * flat_hot, 1)).astype(jnp.int32)
    room = N_EP * CAP
    slot_index = (flat_ids * room + slot_rank).astype(jnp.int32)
    slot_table = jnp.full((EXPERTS * room,), TOKENS * TOP, jnp.int32).at[slot_index].set(jnp.arange(TOKENS * TOP, dtype=jnp.int32))
    padded_in = jnp.concatenate([mlp_in, jnp.zeros((1, D), jnp.float32)], 0)
    rows_in = low_back(padded_in[(slot_table // TOP).astype(jnp.int32)]).reshape(EXPERTS, room, D)
    rows_out = lax.map(expert_block, (rows_in, expert_gate, expert_up, expert_down)).reshape(EXPERTS * room, D)
    picked_rows = rows_out[slot_index].reshape(TOKENS, TOP, D)
    gate_values = jnp.take_along_axis(router_probs, routes.astype(jnp.int32), axis=1)
    mixture = jnp.einsum('sk,skd->sd', gate_values, picked_rows, precision=lax.Precision.HIGHEST)
    share_gate_pre = low_back(matmul(mlp_in, shared_gate))
    share_up_pre = low_back(matmul(mlp_in, shared_up))
    shared_inner = low(share_gate_pre * lax.logistic(share_gate_pre) * share_up_pre)
    shared_out = low_back(matmul(shared_inner, shared_down))
    switch_logit = low_back(matmul(mlp_in, shared_switch))
    block_result = hidden_state + mixture + lax.logistic(switch_logit)[:, None] * shared_out
    expert_counts = lax.optimization_barrier(jnp.sum(live_rows[:, None] * lax.optimization_barrier(jnp.sum(flat_hot.reshape(TOKENS, TOP, EXPERTS), 1)).astype(jnp.float32), 0))
    live_total = jnp.sum(live_rows)
    prob_sums = lax.optimization_barrier(jnp.sum(live_rows[:, None] * router_probs, 0))
    aux_loss = EXPERTS * jnp.sum(expert_counts / live_total * prob_sums / live_total)
    return (block_result, aux_loss)

def reference(tokens, lengths, routes, attention_gain, query_weight, key_weight, value_weight, query_bias, key_bias, value_bias, output_weight, feedforward_gain, router_weight, shared_switch, shared_gate, shared_up, shared_down, expert_gate, expert_up, expert_down, cotangent):
    primals = (tokens, attention_gain, query_weight, key_weight, value_weight, query_bias, key_bias, value_bias, output_weight, feedforward_gain, router_weight, shared_switch, shared_gate, shared_up, shared_down, expert_gate, expert_up, expert_down)
    primals = tuple((item.astype(jnp.float32) for item in primals))

    def run_layer(*params):
        return forward(*params, routes, lengths)
    (block_result, aux_loss), pullback = jax.vjp(run_layer, *primals)
    grad_out = cotangent.astype(jnp.float32) * live_mask(lengths)[:, None]
    gradient = pullback((grad_out, jnp.asarray(aux_weight, dtype=aux_loss.dtype)))
    expert_load = load_counts(routes, lengths)
    return (block_result.astype(jnp.bfloat16), aux_loss, expert_load, gradient[0], gradient[1], gradient[2], gradient[3], gradient[4], gradient[5], gradient[6], gradient[7], gradient[8], gradient[9], gradient[10], gradient[11], gradient[12], gradient[13], gradient[14], gradient[15], gradient[16], gradient[17])
```

```python
import jax
import jax.numpy as jnp
from jax import lax
from jax.sharding import PartitionSpec as P

epsilon = 1e-06
rope_base = 1000000.0
aux_weight = 0.001


def rotation_tables(slot_count, head_size):
    half_size = head_size // 2
    frequency = rope_base ** (-jnp.arange(half_size, dtype=jnp.float32) * 2.0 / head_size)
    angles = jnp.arange(slot_count, dtype=jnp.float32)[:, None] * frequency[None, :]
    cosine = jnp.concatenate([jnp.cos(angles), jnp.cos(angles)], -1)[:, None, :]
    sine_table = jnp.concatenate([jnp.sin(angles), jnp.sin(angles)], -1)[:, None, :]
    return (cosine, sine_table)


def rotate(values, cosine, sine_table):
    half_size = values.shape[-1] // 2
    turned = jnp.concatenate([-values[..., half_size:], values[..., :half_size]], -1)
    return values * cosine + turned * sine_table


def rotate_back(gradient, cosine, sine_table):
    half_size = gradient.shape[-1] // 2
    scaled = gradient * sine_table
    turned = jnp.concatenate([scaled[..., half_size:], -scaled[..., :half_size]], -1)
    return gradient * cosine + turned


def silu_parts(values):
    logistic_vals = lax.logistic(values)
    return (values * logistic_vals, logistic_vals * (1.0 + values * (1.0 - logistic_vals)))


def join_features(arrived):
    return lax.all_gather(arrived, "tp", axis=2, tiled=True)


def send_rows(buffer):
    return lax.all_to_all(buffer, "ep", split_axis=0, concat_axis=0, tiled=True)


def send_home(partial_value):
    summed_rows = lax.psum_scatter(partial_value, "tp", scatter_dimension=2, tiled=True).astype(
        jnp.bfloat16
    )
    arrived = lax.all_to_all(summed_rows, "ep", split_axis=0, concat_axis=0, tiled=True)
    return join_features(arrived)


def slot_shards(
    tokens,
    lengths,
    routes,
    attention_gain,
    query_weight,
    key_weight,
    value_weight,
    query_bias,
    key_bias,
    value_bias,
    output_weight,
    feedforward_gain,
    router_weight,
    shared_switch,
    shared_gate,
    shared_up,
    shared_down,
    expert_gate,
    expert_up,
    expert_down,
    cotangent,
):
    single_float32 = jnp.float32
    brain_float16 = jnp.bfloat16
    (
        attention_gain,
        query_weight,
        key_weight,
        value_weight,
        query_bias,
        key_bias,
        value_bias,
        output_weight,
        feedforward_gain,
        router_weight,
        shared_switch,
        shared_gate,
        shared_up,
        shared_down,
    ) = (
        lax.all_gather(attention_gain, "ep", axis=0, tiled=True),
        lax.all_gather(query_weight, "ep", axis=0, tiled=True),
        lax.all_gather(key_weight, "ep", axis=0, tiled=True),
        lax.all_gather(value_weight, "ep", axis=0, tiled=True),
        lax.all_gather(query_bias, "ep", axis=1, tiled=True),
        lax.all_gather(key_bias, "ep", axis=1, tiled=True),
        lax.all_gather(value_bias, "ep", axis=1, tiled=True),
        lax.all_gather(output_weight, "ep", axis=1, tiled=True),
        lax.all_gather(feedforward_gain, "ep", axis=0, tiled=True),
        lax.all_gather(router_weight, "ep", axis=0, tiled=True),
        lax.all_gather(shared_switch, "ep", axis=0, tiled=True),
        lax.all_gather(shared_gate, "ep", axis=0, tiled=True),
        lax.all_gather(shared_up, "ep", axis=0, tiled=True),
        lax.all_gather(shared_down, "ep", axis=1, tiled=True),
    )
    slot_count = tokens.shape[0]
    model_width = tokens.shape[1]
    top_count = routes.shape[1]
    experts = router_weight.shape[1]
    heads_here = query_bias.shape[0]
    head_size = query_bias.shape[1]
    owners = lax.axis_size("ep")
    per_owner = expert_gate.shape[0]
    capacity = 3 * slot_count * top_count // (2 * experts)
    seq_length = lengths[0]
    positions = jnp.arange(slot_count, dtype=jnp.int32)
    live_rows = (positions < seq_length).astype(single_float32)
    inputs = tokens.astype(single_float32)
    scale_one = lax.rsqrt(jnp.mean(inputs * inputs, -1, keepdims=True) + epsilon)
    normed_one = inputs * scale_one
    attn_in = (normed_one * attention_gain.astype(single_float32)).astype(brain_float16)
    query_pre = jnp.dot(
        attn_in, query_weight, preferred_element_type=single_float32
    ) + query_bias.reshape(-1).astype(single_float32)
    key_pre = jnp.dot(
        attn_in, key_weight, preferred_element_type=single_float32
    ) + key_bias.reshape(-1).astype(single_float32)
    value_pre = jnp.dot(
        attn_in, value_weight, preferred_element_type=single_float32
    ) + value_bias.reshape(-1).astype(single_float32)
    cosine, sine_table = rotation_tables(slot_count, head_size)
    head_shape = (slot_count, heads_here, head_size)
    queries = rotate(query_pre.reshape(head_shape), cosine, sine_table).astype(brain_float16)
    key_heads = rotate(key_pre.reshape(head_shape), cosine, sine_table).astype(brain_float16)
    value_heads = value_pre.astype(brain_float16).reshape(head_shape)
    score_scale = head_size ** (-0.5)
    keep_mask = (positions[None, :] <= positions[:, None]) & (positions[None, :] < seq_length)
    scores = (
        jnp.einsum("shd,thd->hst", queries, key_heads, preferred_element_type=single_float32)
        * score_scale
    )
    scores = jnp.where(keep_mask[None], scores, -1e30)
    top_score = jnp.max(scores, -1, keepdims=True)
    exp_scores = jnp.exp(scores - top_score)
    row_total = jnp.sum(exp_scores, -1, keepdims=True)
    attn_probs = exp_scores / row_total
    log_total = top_score + jnp.log(row_total)
    mixed_heads = (
        jnp.einsum(
            "hst,thd->shd",
            attn_probs.astype(brain_float16),
            value_heads,
            preferred_element_type=single_float32,
        )
        .astype(brain_float16)
        .reshape(slot_count, -1)
    )
    attn_out = lax.psum(
        jnp.dot(mixed_heads, output_weight, preferred_element_type=single_float32), "tp"
    )
    hidden_state = inputs + attn_out
    scale_two = lax.rsqrt(jnp.mean(hidden_state * hidden_state, -1, keepdims=True) + epsilon)
    normed_two = hidden_state * scale_two
    mlp_in = (normed_two * feedforward_gain.astype(single_float32)).astype(brain_float16)
    logits = jnp.dot(mlp_in, router_weight, preferred_element_type=single_float32)
    top_logit = jnp.max(logits, -1, keepdims=True)
    exp_logits = jnp.exp(logits - top_logit)
    router_probs = exp_logits / jnp.sum(exp_logits, -1, keepdims=True)
    expert_ids = jnp.arange(experts, dtype=jnp.int32)
    chosen = (routes[:, :, None] == expert_ids[None, None, :]).astype(single_float32)
    gate_values = jnp.sum(chosen * router_probs[:, None, :], -1)
    expert_counts = jnp.sum(live_rows[:, None] * jnp.sum(chosen, 1), 0)
    prob_sums = jnp.sum(live_rows[:, None] * router_probs, 0)
    expert_counts, prob_sums, live_total = lax.psum(
        (expert_counts, prob_sums, jnp.sum(live_rows)), "ep"
    )
    aux_loss = experts * jnp.sum(expert_counts / live_total * prob_sums / live_total)
    flat_ids = routes.reshape(-1)
    flat_hot = (flat_ids[:, None] == expert_ids[None, :]).astype(jnp.int32)
    slot_rank = jnp.sum((jnp.cumsum(flat_hot, 0) - flat_hot) * flat_hot, 1)
    slot_index = flat_ids * capacity + slot_rank
    row_count = slot_count * top_count
    slot_table = (
        jnp.full((experts * capacity,), row_count, jnp.int32)
        .at[slot_index]
        .set(jnp.arange(row_count, dtype=jnp.int32))
    )
    send_shape = (owners, per_owner * capacity, model_width)
    grid_shape = (owners, per_owner, capacity, model_width)
    padded_in = jnp.concatenate([mlp_in, jnp.zeros((1, model_width), brain_float16)], 0)
    send_buffer = padded_in[slot_table // top_count]
    gate_matrix, up_weight_matrix, down_matrix = (expert_gate, expert_up, expert_down)
    received_rows = send_rows(send_buffer.reshape(send_shape)).reshape(grid_shape)
    gate_hidden = jnp.einsum(
        "necd,edf->necf", received_rows, gate_matrix, preferred_element_type=single_float32
    )
    up_hidden = jnp.einsum(
        "necd,edf->necf", received_rows, up_weight_matrix, preferred_element_type=single_float32
    )
    activated_gate, slope_gate = silu_parts(gate_hidden)
    inner_act = (activated_gate * up_hidden).astype(brain_float16)
    expert_part = jnp.einsum(
        "necf,efd->necd", inner_act, down_matrix, preferred_element_type=single_float32
    )
    returned = send_home(expert_part.reshape(send_shape))
    returned = returned.reshape(experts * capacity, model_width)
    picked_rows = returned[slot_index].reshape(slot_count, top_count, model_width)
    mixture = jnp.sum(gate_values[:, :, None] * picked_rows.astype(single_float32), 1)
    share_gate_pre = jnp.dot(mlp_in, shared_gate, preferred_element_type=single_float32)
    share_up_pre = jnp.dot(mlp_in, shared_up, preferred_element_type=single_float32)
    share_act, share_slope = silu_parts(share_gate_pre)
    shared_inner = (share_act * share_up_pre).astype(brain_float16)
    shared_out = lax.psum(
        jnp.dot(shared_inner, shared_down, preferred_element_type=single_float32).astype(
            jnp.bfloat16
        ),
        "tp",
    ).astype(jnp.float32)
    switch_logit = jnp.dot(mlp_in, shared_switch, preferred_element_type=single_float32)
    switch = lax.logistic(switch_logit)
    block_result = hidden_state + mixture + switch[:, None] * shared_out
    output = block_result.astype(brain_float16)
    grad_out = cotangent.astype(single_float32) * live_rows[:, None]
    grad_share = (grad_out * switch[:, None]).astype(brain_float16)
    grad_switch = (jnp.sum(grad_out * shared_out, -1) * switch * (1.0 - switch)).astype(
        brain_float16
    )
    shared_down_grad = jnp.dot(shared_inner.T, grad_share, preferred_element_type=single_float32)
    grad_shared_inner = jnp.dot(grad_share, shared_down.T, preferred_element_type=single_float32)
    grad_sgate = (grad_shared_inner * share_up_pre * share_slope).astype(brain_float16)
    grad_sup = (grad_shared_inner * share_act).astype(brain_float16)
    shared_gate_grad = jnp.dot(mlp_in.T, grad_sgate, preferred_element_type=single_float32)
    shared_up_grad = jnp.dot(mlp_in.T, grad_sup, preferred_element_type=single_float32)
    shared_switch_grad = jnp.dot(grad_switch, mlp_in, preferred_element_type=single_float32)
    shared_back = lax.psum(
        (
            jnp.dot(grad_sgate, shared_gate.T, preferred_element_type=single_float32)
            + jnp.dot(grad_sup, shared_up.T, preferred_element_type=single_float32)
        ).astype(jnp.bfloat16),
        "tp",
    ).astype(jnp.float32)
    gate_grad = jnp.sum(grad_out[:, None, :] * picked_rows.astype(single_float32), -1)
    grad_rows = (
        (gate_values[:, :, None] * grad_out[:, None, :])
        .astype(brain_float16)
        .reshape(row_count, model_width)
    )
    padded_grad = jnp.concatenate([grad_rows, jnp.zeros((1, model_width), brain_float16)], 0)
    grad_buffer = padded_grad[slot_table]
    grad_received = send_rows(grad_buffer.reshape(send_shape)).reshape(grid_shape)
    expert_inner_gradient = jnp.einsum(
        "necd,efd->necf", grad_received, down_matrix, preferred_element_type=single_float32
    )
    grad_egate = (expert_inner_gradient * up_hidden * slope_gate).astype(brain_float16)
    expert_up_partial = (expert_inner_gradient * activated_gate).astype(brain_float16)
    expert_down_grad = jnp.einsum(
        "necf,necd->efd", inner_act, grad_received, preferred_element_type=single_float32
    )
    expert_gate_grad = jnp.einsum(
        "uxvp,uxvh->xph", received_rows, grad_egate, preferred_element_type=single_float32
    )
    expert_up_gradient = jnp.einsum(
        "uxvp,uxvh->xph", received_rows, expert_up_partial, preferred_element_type=single_float32
    )
    grad_back_rows = jnp.einsum(
        "kqib,qzb->kqiz", grad_egate, gate_matrix, preferred_element_type=single_float32
    ) + jnp.einsum(
        "kqib,qzb->kqiz", expert_up_partial, up_weight_matrix, preferred_element_type=single_float32
    )
    home_grad = send_home(grad_back_rows.reshape(send_shape))
    home_grad = home_grad.reshape(experts * capacity, model_width)
    expert_back = jnp.sum(
        home_grad[slot_index].reshape(slot_count, top_count, model_width).astype(single_float32), 1
    )
    grad_probs = (
        jnp.sum(chosen * gate_grad[:, :, None], 1)
        + aux_weight
        * experts
        * (expert_counts / (live_total * live_total))[None, :]
        * live_rows[:, None]
    )
    grad_logits = (
        router_probs * (grad_probs - jnp.sum(router_probs * grad_probs, -1, keepdims=True))
    ).astype(brain_float16)
    router_weight_grad = jnp.dot(mlp_in.T, grad_logits, preferred_element_type=single_float32)
    grad_mlp_in = (
        shared_back
        + expert_back
        + jnp.dot(grad_logits, router_weight.T, preferred_element_type=single_float32)
        + grad_switch.astype(single_float32)[:, None]
        * shared_switch.astype(single_float32)[None, :]
    )
    grad_norm_two = grad_mlp_in * feedforward_gain.astype(single_float32)
    feedforward_gain_grad = jnp.sum(grad_mlp_in * normed_two, 0)
    grad_hidden = grad_out + scale_two * (
        grad_norm_two - normed_two * jnp.mean(grad_norm_two * normed_two, -1, keepdims=True)
    )
    grad_branch = grad_hidden.astype(brain_float16)
    output_weight_grad = jnp.dot(mixed_heads.T, grad_branch, preferred_element_type=single_float32)
    grad_mixed = (
        jnp.dot(grad_branch, output_weight.T, preferred_element_type=single_float32)
        .astype(brain_float16)
        .reshape(head_shape)
    )
    grad_weights = jnp.einsum(
        "shd,thd->hst", grad_mixed, value_heads, preferred_element_type=single_float32
    )
    scores_again = (
        jnp.einsum("shd,thd->hst", queries, key_heads, preferred_element_type=single_float32)
        * score_scale
    )
    scores_again = jnp.where(keep_mask[None], scores_again, -1e30)
    probs_again = jnp.exp(scores_again - log_total)
    row_delta = jnp.sum(probs_again * grad_weights, -1, keepdims=True)
    grad_scores = (probs_again * (grad_weights - row_delta)).astype(brain_float16)
    grad_value = (
        jnp.einsum(
            "hst,shd->thd",
            probs_again.astype(brain_float16),
            grad_mixed,
            preferred_element_type=single_float32,
        )
        .astype(brain_float16)
        .reshape(slot_count, -1)
    )
    grad_queries = (
        jnp.einsum("hst,thd->shd", grad_scores, key_heads, preferred_element_type=single_float32)
        * score_scale
    )
    grad_keys = (
        jnp.einsum("hst,shd->thd", grad_scores, queries, preferred_element_type=single_float32)
        * score_scale
    )
    grad_query = (
        rotate_back(grad_queries, cosine, sine_table).astype(brain_float16).reshape(slot_count, -1)
    )
    grad_key = (
        rotate_back(grad_keys, cosine, sine_table).astype(brain_float16).reshape(slot_count, -1)
    )
    query_weight_grad = jnp.dot(attn_in.T, grad_query, preferred_element_type=single_float32)
    key_weight_grad = jnp.dot(attn_in.T, grad_key, preferred_element_type=single_float32)
    value_weight_grad = jnp.dot(attn_in.T, grad_value, preferred_element_type=single_float32)
    query_bias_grad = jnp.sum(grad_query.astype(single_float32), 0).reshape(heads_here, head_size)
    key_bias_grad = jnp.sum(grad_key.astype(single_float32), 0).reshape(heads_here, head_size)
    value_bias_grad = jnp.sum(grad_value.astype(single_float32), 0).reshape(heads_here, head_size)
    grad_attn_in = lax.psum(
        (
            jnp.dot(grad_query, query_weight.T, preferred_element_type=single_float32)
            + jnp.dot(grad_key, key_weight.T, preferred_element_type=single_float32)
            + jnp.dot(grad_value, value_weight.T, preferred_element_type=single_float32)
        ).astype(jnp.bfloat16),
        "tp",
    ).astype(jnp.float32)
    grad_norm_one = grad_attn_in * attention_gain.astype(single_float32)
    attention_gain_grad = jnp.sum(grad_attn_in * normed_one, 0)
    tokens_grad = grad_hidden + scale_one * (
        grad_norm_one - normed_one * jnp.mean(grad_norm_one * normed_one, -1, keepdims=True)
    )
    reduced = (
        lax.psum_scatter(
            attention_gain_grad.astype(jnp.bfloat16), "ep", scatter_dimension=0, tiled=True
        ).astype(jnp.float32),
        lax.psum_scatter(
            query_weight_grad.astype(jnp.bfloat16), "ep", scatter_dimension=0, tiled=True
        ).astype(jnp.float32),
        lax.psum_scatter(
            key_weight_grad.astype(jnp.bfloat16), "ep", scatter_dimension=0, tiled=True
        ).astype(jnp.float32),
        lax.psum_scatter(
            value_weight_grad.astype(jnp.bfloat16), "ep", scatter_dimension=0, tiled=True
        ).astype(jnp.float32),
        lax.psum_scatter(
            query_bias_grad.astype(jnp.bfloat16), "ep", scatter_dimension=1, tiled=True
        ).astype(jnp.float32),
        lax.psum_scatter(
            key_bias_grad.astype(jnp.bfloat16), "ep", scatter_dimension=1, tiled=True
        ).astype(jnp.float32),
        lax.psum_scatter(
            value_bias_grad.astype(jnp.bfloat16), "ep", scatter_dimension=1, tiled=True
        ).astype(jnp.float32),
        lax.psum_scatter(
            output_weight_grad.astype(jnp.bfloat16), "ep", scatter_dimension=1, tiled=True
        ).astype(jnp.float32),
        lax.psum_scatter(
            feedforward_gain_grad.astype(jnp.bfloat16), "ep", scatter_dimension=0, tiled=True
        ).astype(jnp.float32),
        lax.psum_scatter(
            router_weight_grad.astype(jnp.bfloat16), "ep", scatter_dimension=0, tiled=True
        ).astype(jnp.float32),
        lax.psum_scatter(
            shared_switch_grad.astype(jnp.bfloat16), "ep", scatter_dimension=0, tiled=True
        ).astype(jnp.float32),
        lax.psum_scatter(
            shared_gate_grad.astype(jnp.bfloat16), "ep", scatter_dimension=0, tiled=True
        ).astype(jnp.float32),
        lax.psum_scatter(
            shared_up_grad.astype(jnp.bfloat16), "ep", scatter_dimension=0, tiled=True
        ).astype(jnp.float32),
        lax.psum_scatter(
            shared_down_grad.astype(jnp.bfloat16), "ep", scatter_dimension=1, tiled=True
        ).astype(jnp.float32),
    )
    return (
        output,
        aux_loss,
        expert_counts,
        tokens_grad,
        reduced[0],
        reduced[1],
        reduced[2],
        reduced[3],
        reduced[4],
        reduced[5],
        reduced[6],
        reduced[7],
        reduced[8],
        reduced[9],
        reduced[10],
        reduced[11],
        reduced[12],
        reduced[13],
        expert_gate_grad,
        expert_up_gradient,
        expert_down_grad,
    )


lane_width = 128


def padded_size(units):
    return -(-units // lane_width) * lane_width


def pad_columns(matrix, width):
    return jnp.pad(matrix, ((0, 0), (0, width - matrix.shape[1])))


def dense_shards(
    tokens,
    lengths,
    routes,
    attention_gain,
    query_weight,
    key_weight,
    value_weight,
    query_bias,
    key_bias,
    value_bias,
    output_weight,
    feedforward_gain,
    router_weight,
    shared_switch,
    shared_gate,
    shared_up,
    shared_down,
    expert_gate,
    expert_up,
    expert_down,
    cotangent,
):
    f32 = jnp.float32
    bf16 = jnp.bfloat16
    owners = lax.axis_size("ep")
    my_expert = lax.axis_index("ep")
    slot_count, model_width = tokens.shape
    top_count = routes.shape[1]
    experts = router_weight.shape[1]
    heads_here, bias_cut = query_bias.shape
    head_size = bias_cut * owners
    head_width = heads_here * head_size
    rows_here = query_weight.shape[0]
    expert_units = expert_gate.shape[2]
    shared_units = shared_gate.shape[1] // owners
    expert_room = padded_size(expert_units)
    shared_room = padded_size(shared_units)
    all_tokens = owners * slot_count

    packed = jnp.concatenate([query_weight, key_weight, value_weight, output_weight.T], 1)
    packed = lax.all_gather(packed, "ep", axis=0, tiled=True)
    qkv_weight = packed[:, : 3 * head_width]
    output_back = packed[:, 3 * head_width :]

    small = [
        attention_gain,
        feedforward_gain,
        shared_switch,
        router_weight.reshape(-1),
        query_bias.reshape(-1),
        key_bias.reshape(-1),
        value_bias.reshape(-1),
        routes.reshape(-1).astype(bf16),
        (lengths // 256).astype(bf16),
        (lengths % 256).astype(bf16),
    ]
    small_sizes = [piece.shape[0] for piece in small]
    small = jnp.concatenate(small)
    small = jnp.pad(small, (0, -small.shape[0] % 1024))
    small = lax.all_gather(small[None], "ep", axis=0, tiled=True)
    pieces = []
    start = 0
    for size in small_sizes:
        pieces.append(small[:, start : start + size])
        start += size
    attn_gain = pieces[0].reshape(model_width).astype(f32)
    ff_gain = pieces[1].reshape(model_width).astype(f32)
    switch_weight = pieces[2].reshape(model_width)
    router = pieces[3].reshape(model_width, experts)
    biases = jnp.stack(pieces[4:7]).reshape(3, owners, heads_here, bias_cut)
    biases = biases.transpose(0, 2, 1, 3).reshape(3 * head_width).astype(f32)
    all_routes = pieces[7].reshape(all_tokens, top_count).astype(jnp.int32)
    all_lengths = pieces[8].astype(f32) * 256 + pieces[9].astype(f32)
    all_lengths = all_lengths.astype(jnp.int32).reshape(owners)

    seq_length = lengths[0]
    positions = jnp.arange(slot_count, dtype=jnp.int32)
    live_rows = (positions < seq_length).astype(f32)
    live_all = (positions[None, :] < all_lengths[:, None]).astype(f32).reshape(all_tokens)
    live_total = jnp.sum(live_all)
    expert_ids = jnp.arange(experts, dtype=jnp.int32)
    chosen_all = jnp.sum((all_routes[:, :, None] == expert_ids).astype(f32), 1)
    chosen = jnp.sum((routes[:, :, None] == expert_ids).astype(f32), 1)
    expert_counts = jnp.sum(live_all[:, None] * chosen_all, 0)

    grad_live = jnp.where(live_rows[:, None] > 0, cotangent, jnp.zeros_like(cotangent))
    grad_out = grad_live.astype(f32)
    grad_all = lax.all_gather(grad_live, "ep", axis=0, tiled=True)

    weight_cuts = jnp.concatenate(
        [
            shared_gate.reshape(rows_here, owners, shared_units).transpose(1, 0, 2),
            shared_up.reshape(rows_here, owners, shared_units).transpose(1, 0, 2),
            shared_down.reshape(owners, shared_units, rows_here).transpose(0, 2, 1),
        ],
        2,
    )
    weight_cuts = lax.all_to_all(weight_cuts, "ep", split_axis=0, concat_axis=0, tiled=True)
    weight_cuts = weight_cuts.reshape(model_width, 3 * shared_units)
    gate_matrix = jnp.concatenate(
        [
            pad_columns(expert_gate[0], expert_room),
            pad_columns(weight_cuts[:, :shared_units], shared_room),
        ],
        1,
    )
    up_matrix = jnp.concatenate(
        [
            pad_columns(expert_up[0], expert_room),
            pad_columns(weight_cuts[:, shared_units : 2 * shared_units], shared_room),
        ],
        1,
    )
    down_matrix = jnp.concatenate(
        [
            jnp.pad(expert_down[0], ((0, expert_room - expert_units), (0, 0))),
            pad_columns(weight_cuts[:, 2 * shared_units :], shared_room).T,
        ],
        0,
    )
    units = expert_room + shared_room

    inputs = tokens.astype(f32)
    scale_one = lax.rsqrt(jnp.mean(inputs * inputs, -1, keepdims=True) + epsilon)
    normed_one = inputs * scale_one
    attn_in = (normed_one * attn_gain).astype(bf16)
    qkv_pre = jnp.dot(attn_in, qkv_weight, preferred_element_type=f32) + biases
    cosine, sine_table = rotation_tables(slot_count, head_size)
    head_shape = (slot_count, heads_here, head_size)
    queries = rotate(qkv_pre[:, :head_width].reshape(head_shape), cosine, sine_table).astype(bf16)
    key_heads = rotate(
        qkv_pre[:, head_width : 2 * head_width].reshape(head_shape), cosine, sine_table
    ).astype(bf16)
    value_heads = qkv_pre[:, 2 * head_width :].astype(bf16).reshape(head_shape)
    score_scale = head_size ** (-0.5)
    keep_mask = (positions[None, :] <= positions[:, None]) & (positions[None, :] < seq_length)
    scores = (
        jnp.einsum("shd,thd->hst", queries, key_heads, preferred_element_type=f32) * score_scale
    )
    scores = jnp.where(keep_mask[None], scores, -1e30)
    top_score = jnp.max(scores, -1, keepdims=True)
    exp_scores = jnp.exp(scores - top_score)
    attn_probs = exp_scores / jnp.sum(exp_scores, -1, keepdims=True)
    probs_low = attn_probs.astype(bf16)
    mixed_heads = (
        jnp.einsum("hst,thd->shd", probs_low, value_heads, preferred_element_type=f32)
        .astype(bf16)
        .reshape(slot_count, head_width)
    )
    attn_out = lax.psum(
        jnp.einsum("sh,dh->sd", mixed_heads, output_back, preferred_element_type=f32).astype(bf16),
        "tp",
    )
    hidden_state = inputs + attn_out.astype(f32)
    scale_two = lax.rsqrt(jnp.mean(hidden_state * hidden_state, -1, keepdims=True) + epsilon)
    normed_two = hidden_state * scale_two
    mlp_in = (normed_two * ff_gain).astype(bf16)
    mlp_all = lax.all_gather(mlp_in, "ep", axis=0, tiled=True)

    router_switch = jnp.concatenate([router, switch_weight[:, None]], 1)

    def routing(rows):
        logits = jnp.dot(rows, router_switch, preferred_element_type=f32)
        return jax.nn.softmax(logits[:, :experts], axis=-1), lax.logistic(logits[:, experts])

    router_probs, switch = routing(mlp_in)
    probs_all, switch_all = routing(mlp_all)
    prob_sums = jnp.sum(live_all[:, None] * probs_all, 0)
    aux_loss = experts * jnp.sum(expert_counts / live_total * prob_sums / live_total)
    mine = (expert_ids == my_expert).astype(f32)
    gate_all = jnp.sum(chosen_all * probs_all * mine, 1)
    in_expert = jnp.arange(units) < expert_room
    row_weight = jnp.where(in_expert[None, :], gate_all[:, None], switch_all[:, None])

    grad_units = jnp.einsum("td,fd->tf", grad_all, down_matrix, preferred_element_type=f32)
    gate_pre = jnp.dot(mlp_all, gate_matrix, preferred_element_type=f32)
    up_pre = jnp.dot(mlp_all, up_matrix, preferred_element_type=f32)
    act, slope = silu_parts(gate_pre)
    inner = act * up_pre
    inner_weighted = (row_weight * inner).astype(bf16)
    weighted_grad = row_weight * grad_units
    grad_gate = (weighted_grad * up_pre * slope).astype(bf16)
    grad_up = (weighted_grad * act).astype(bf16)
    unit_products = inner * grad_units
    gate_sum = jnp.sum(unit_products[:, :expert_room], -1)
    switch_sum = jnp.sum(unit_products[:, expert_room:], -1)

    result_part = jnp.dot(inner_weighted, down_matrix, preferred_element_type=f32).astype(bf16)
    result_part = lax.psum_scatter(result_part, "ep", scatter_dimension=0, tiled=True)

    extra_ids = jnp.arange(lane_width, dtype=jnp.int32)
    extra = jnp.where(extra_ids == my_expert, gate_sum[:, None], 0.0) + jnp.where(
        extra_ids == experts, switch_sum[:, None], 0.0
    )
    back_part = jnp.einsum(
        "tf,df->td",
        jnp.concatenate([grad_gate, grad_up], 1),
        jnp.concatenate([gate_matrix, up_matrix], 1),
        preferred_element_type=f32,
    ).astype(bf16)
    back_part = jnp.concatenate([back_part, extra.astype(bf16)], 1)
    back_part = lax.psum_scatter(back_part, "ep", scatter_dimension=0, tiled=True)
    back = lax.psum(back_part, "tp").astype(f32)
    result_sum = lax.psum(result_part, "tp").astype(f32)
    output = (hidden_state + result_sum).astype(bf16)

    gate_weight_grad = jnp.einsum("td,tf->df", mlp_all, grad_gate, preferred_element_type=f32)
    up_weight_grad = jnp.einsum("td,tf->df", mlp_all, grad_up, preferred_element_type=f32)
    down_weight_grad = jnp.einsum(
        "tf,td->fd", inner_weighted, grad_all, preferred_element_type=f32
    )
    shared_cut = slice(expert_room, expert_room + shared_units)
    grad_cuts = jnp.concatenate(
        [
            gate_weight_grad[:, shared_cut].astype(bf16),
            up_weight_grad[:, shared_cut].astype(bf16),
            down_weight_grad[shared_cut].astype(bf16).T,
        ],
        1,
    ).reshape(owners, rows_here, 3 * shared_units)
    grad_cuts = lax.all_to_all(grad_cuts, "ep", split_axis=0, concat_axis=0, tiled=True)
    grad_cuts = grad_cuts.reshape(owners, rows_here, 3, shared_units)
    shared_gate_grad = grad_cuts[:, :, 0].transpose(1, 0, 2).reshape(shared_gate.shape).astype(f32)
    shared_up_grad = grad_cuts[:, :, 1].transpose(1, 0, 2).reshape(shared_up.shape).astype(f32)
    shared_down_grad = (
        grad_cuts[:, :, 2].transpose(0, 2, 1).reshape(shared_down.shape).astype(f32)
    )

    gate_grad = back[:, model_width : model_width + experts]
    grad_switch = (back[:, model_width + experts] * switch * (1.0 - switch)).astype(bf16)
    grad_probs = (
        chosen * gate_grad
        + aux_weight
        * experts
        * (expert_counts / (live_total * live_total))[None, :]
        * live_rows[:, None]
    )
    grad_logits = (
        router_probs * (grad_probs - jnp.sum(router_probs * grad_probs, -1, keepdims=True))
    ).astype(bf16)
    grad_choices = jnp.concatenate([grad_logits, grad_switch[:, None]], 1)
    choice_weight_grad = jnp.einsum("td,te->de", mlp_in, grad_choices, preferred_element_type=f32)
    grad_mlp_in = back[:, :model_width] + jnp.einsum(
        "te,de->td", grad_choices, router_switch, preferred_element_type=f32
    )
    grad_norm_two = grad_mlp_in * ff_gain
    feedforward_gain_grad = jnp.sum(grad_mlp_in * normed_two, 0)
    grad_hidden = grad_out + scale_two * (
        grad_norm_two - normed_two * jnp.mean(grad_norm_two * normed_two, -1, keepdims=True)
    )
    grad_branch = grad_hidden.astype(bf16)
    output_weight_grad = jnp.einsum(
        "sd,sh->dh", grad_branch, mixed_heads, preferred_element_type=f32
    )
    grad_mixed = (
        jnp.dot(grad_branch, output_back, preferred_element_type=f32)
        .astype(bf16)
        .reshape(head_shape)
    )
    grad_weights = jnp.einsum("shd,thd->hst", grad_mixed, value_heads, preferred_element_type=f32)
    row_delta = jnp.sum(attn_probs * grad_weights, -1, keepdims=True)
    grad_scores = (attn_probs * (grad_weights - row_delta)).astype(bf16)
    grad_value = (
        jnp.einsum("hst,shd->thd", probs_low, grad_mixed, preferred_element_type=f32)
        .astype(bf16)
        .reshape(slot_count, head_width)
    )
    grad_queries = (
        jnp.einsum("hst,thd->shd", grad_scores, key_heads, preferred_element_type=f32)
        * score_scale
    )
    grad_keys = (
        jnp.einsum("hst,shd->thd", grad_scores, queries, preferred_element_type=f32) * score_scale
    )
    grad_query = rotate_back(grad_queries, cosine, sine_table).astype(bf16)
    grad_key = rotate_back(grad_keys, cosine, sine_table).astype(bf16)
    grad_qkv = jnp.concatenate(
        [
            grad_query.reshape(slot_count, head_width),
            grad_key.reshape(slot_count, head_width),
            grad_value,
        ],
        1,
    )
    qkv_weight_grad = jnp.einsum("td,th->dh", attn_in, grad_qkv, preferred_element_type=f32)
    bias_grads = jnp.sum(grad_qkv.astype(f32), 0)
    grad_attn_part = jnp.einsum("th,dh->td", grad_qkv, qkv_weight, preferred_element_type=f32)
    attention_gain_part = jnp.sum(grad_attn_part * normed_one, 0)
    grad_attn_in = lax.psum(grad_attn_part.astype(bf16), "tp").astype(f32)
    grad_norm_one = grad_attn_in * attn_gain
    tokens_grad = grad_hidden + scale_one * (
        grad_norm_one - normed_one * jnp.mean(grad_norm_one * normed_one, -1, keepdims=True)
    )

    dense_grads = jnp.concatenate(
        [qkv_weight_grad.astype(bf16), output_weight_grad.astype(bf16)], 1
    )
    dense_grads = lax.psum_scatter(dense_grads, "ep", scatter_dimension=0, tiled=True).astype(f32)
    bias_grads = bias_grads.reshape(3, heads_here, owners, bias_cut).transpose(2, 0, 1, 3)
    small_grads = jnp.concatenate(
        [
            attention_gain_part.reshape(owners, -1),
            feedforward_gain_grad.reshape(owners, -1),
            choice_weight_grad[:, experts].reshape(owners, -1),
            choice_weight_grad[:, :experts].reshape(owners, -1),
            bias_grads.reshape(owners, -1),
        ],
        1,
    )
    small_grads = jnp.pad(small_grads, ((0, 0), (0, -small_grads.shape[1] % 1024)))
    small_grads = lax.all_to_all(small_grads, "ep", split_axis=0, concat_axis=0, tiled=True)
    small_grads = jnp.sum(small_grads, 0)
    attention_gain_grad = lax.psum(small_grads[:rows_here], "tp")
    bias_at = (3 + experts) * rows_here
    bias_rows = small_grads[bias_at : bias_at + 3 * heads_here * bias_cut]
    bias_rows = bias_rows.reshape(3, heads_here, bias_cut)
    return (
        output,
        aux_loss,
        expert_counts,
        tokens_grad,
        attention_gain_grad,
        dense_grads[:, :head_width],
        dense_grads[:, head_width : 2 * head_width],
        dense_grads[:, 2 * head_width : 3 * head_width],
        bias_rows[0],
        bias_rows[1],
        bias_rows[2],
        dense_grads[:, 3 * head_width : 4 * head_width].T,
        small_grads[rows_here : 2 * rows_here],
        small_grads[3 * rows_here : bias_at].reshape(rows_here, experts),
        small_grads[2 * rows_here : 3 * rows_here],
        shared_gate_grad,
        shared_up_grad,
        shared_down_grad,
        gate_weight_grad[None, :, :expert_units],
        up_weight_grad[None, :, :expert_units],
        down_weight_grad[None, :expert_units],
    )


def layer_shards(*arrays):
    routes, router_weight, expert_gate = arrays[2], arrays[12], arrays[17]
    slot_count, top_count = routes.shape
    experts = router_weight.shape[1]
    capacity = 3 * slot_count * top_count // (2 * experts)
    one_each = expert_gate.shape[0] == 1 and experts < lane_width
    if one_each and 2 * capacity >= slot_count:
        return dense_shards(*arrays)
    return slot_shards(*arrays)


def solution(mesh):
    return jax.shard_map(
        layer_shards,
        mesh=mesh,
        in_specs=(
            P("ep", None),
            P("ep"),
            P("ep", None),
            P("ep"),
            P("ep", "tp"),
            P("ep", "tp"),
            P("ep", "tp"),
            P("tp", "ep"),
            P("tp", "ep"),
            P("tp", "ep"),
            P("tp", "ep"),
            P("ep"),
            P("ep", None),
            P("ep"),
            P("ep", "tp"),
            P("ep", "tp"),
            P("tp", "ep"),
            P("ep", None, "tp"),
            P("ep", None, "tp"),
            P("ep", "tp", None),
            P("ep", None),
        ),
        out_specs=(
            P("ep", None),
            P(),
            P(),
            P("ep", None),
            P("ep"),
            P("ep", "tp"),
            P("ep", "tp"),
            P("ep", "tp"),
            P("tp", "ep"),
            P("tp", "ep"),
            P("tp", "ep"),
            P("tp", "ep"),
            P("ep"),
            P("ep", None),
            P("ep"),
            P("ep", "tp"),
            P("ep", "tp"),
            P("tp", "ep"),
            P("ep", None, "tp"),
            P("ep", None, "tp"),
            P("ep", "tp", None),
        ),
        check_vma=False,
    )
```
